32 devices in a mesh: chain: 2 (over y), gz: 4 (over z), gy: 2 (over x), pa: 2 (over core).
Axes of the slice: x: 2, y: 2, z: 4, core: 2. Of those that a mesh axis runs over, the one named last changes fastest.
Arguments:
- probes: float32 [32, 32, 64, 256], P(('chain', 'pa'), 'gz', 'gy'), parts along dimension 0, may hold values from -6 to 6
- velocity: float32 [3, 64, 64, 256], P(None, ('chain', 'gz'), 'gy'), parts along dimension 1, may hold values from -0.3 to 0.3
- prior_scale: float32 [64, 64, 256], P(('chain', 'gz'), 'gy'), parts along dimension 0, may hold values from 0.3 to 3
- noise_precision: float32 [64, 64, 256], P(('chain', 'gz'), 'gy'), parts along dimension 0, may hold values from 0.3 to 3
- source_mask: int32 [64, 64, 256], P(('chain', 'gz'), 'gy'), parts along dimension 0, may hold values 0 or 1
- sensor_mask: int32 [64, 64, 256], P(('chain', 'gz'), 'gy'), parts along dimension 0, may hold values 0 or 1
Outputs:
- hessian: float32 [32, 32, 64, 256], P(('chain', 'pa'), 'gz', 'gy'), parts along dimension 0
- gram: float32 [32, 16], P(('chain', 'pa')), parts along dimension 0
The draws below stay inside these ranges and needn't reach their ends.
There are 2 independent parts, one for each index of `chain`. The reference program is written for one: setup_inputs(seed, part) draws one part's arguments, and reference() takes and returns one part's arrays. A program takes and returns all parts, laid end to end along the dimension named above; each array names one. Nothing has to cross between parts.
All inputs are finite; a program needn't handle non-finite values. No bound on the sum of `source_mask` or of `sensor_mask` on one device may be relied on, other than what follows from the above.
Results may differ from the reference program's by a relative error of at most 0.0003.
Values sent between devices are 32-bit elements; how exact they have to be, the bound alone decides.
A program may use at most 128 MiB of HBM per device.

```python
import math
import jax
import jax.numpy as jnp
from jax import lax

NX = 256
P_SIZE = 16
STEPS = 5
NY = 64
NZ = 32


def touch_ends(values, rng, low, largest):
    longest = values.shape.index(max(values.shape))
    spots = []
    for shift in (0, 1):
        where = [jax.random.randint(jax.random.fold_in(rng, axis), (), 0, length) for axis, length in enumerate(values.shape)]
        where[longest] = (where[longest] + shift) % values.shape[longest]
        spots.append(tuple(where))
    return values.at[spots[0]].set(low).at[spots[1]].set(largest)


def block_scale(rng, extent, shards, low, high):
    level = 1.0
    for dim, parts in shards:
        heights = jax.random.uniform(jax.random.fold_in(jax.random.fold_in(rng, 6), dim), (parts,), jnp.float32, low / len(shards), high / len(shards))
        level = level * jnp.repeat(jnp.exp(heights), extent[dim] // parts).reshape((-1,) + (1,) * (len(extent) - 1 - dim))
    return level


def scatter_about(own_key, shape, deviation, bound, cuts=(), kind=jnp.bfloat16):
    drawn = deviation * jax.random.normal(own_key, shape, jnp.float32)
    if cuts:
        drawn = drawn * block_scale(own_key, shape, cuts, -0.22, 0.18)
    return jnp.clip(drawn, -bound, bound).astype(kind)


def setup_inputs(seed: int = 0, part: int = 0) -> dict:
    splits = jax.random.split(jax.random.key(seed), 7)
    own_keys = jax.random.split(jax.random.fold_in(splits[6], part), 7)
    probes = scatter_about(own_keys[0], (P_SIZE, NZ, NY, NX), 1.0, 6.0, ((0, 2), (1, 4), (2, 2)), jnp.float32)
    velocity = jnp.clip(jax.random.uniform(own_keys[1], (3, NZ, NY, NX), jnp.float32, -0.3, 0.3) * block_scale(own_keys[1], (3, NZ, NY, NX), ((1, 4), (2, 2)), -0.4, 0.0), -0.3, 0.3)
    prior_scale = jnp.clip(jnp.exp(math.log(3.0) - 2.3025851 * jax.random.uniform(own_keys[2], (NZ, NY, NX), jnp.float32) ** block_scale(own_keys[2], (NZ, NY, NX), ((0, 4), (1, 2)), -0.2, 0.2)), 0.3, 3.0)
    noise_precision = jnp.clip(jnp.exp(math.log(3.0) - 2.3025851 * jax.random.uniform(own_keys[3], (NZ, NY, NX), jnp.float32) ** block_scale(own_keys[3], (NZ, NY, NX), ((0, 4), (1, 2)), -0.2, 0.2)), 0.3, 3.0)
    source_mask = touch_ends((jax.random.randint(own_keys[4], (NZ, NY, NX), 0, 2) < 1).astype(jnp.int32), jax.random.fold_in(own_keys[4], 1), 0, 1)
    sensor_mask = touch_ends((jax.random.randint(own_keys[5], (NZ, NY, NX), 0, 4) < 1).astype(jnp.int32), jax.random.fold_in(own_keys[5], 1), 0, 1)
    return {"probes": probes, "velocity": velocity, "prior_scale": prior_scale, "noise_precision": noise_precision, "source_mask": source_mask, "sensor_mask": sensor_mask}


diffuse_cross = 0.15
diffuse_along = 16.0

def shift_cells(field, offset):
    zeros = jnp.zeros(field.shape[:-1] + (1,), jnp.float32)
    if offset > 0:
        return jnp.concatenate([field[..., 1:], zeros], -1)
    return jnp.concatenate([zeros, field[..., :-1]], -1)

def apply_implicit(field, matrix):
    flat = field.reshape(-1, field.shape[-1])
    return jnp.dot(flat.astype(jnp.float32), matrix.astype(jnp.float32), precision=lax.Precision.HIGHEST, preferred_element_type=jnp.float32).reshape(field.shape)

def forward_explicit(padded, coef_pad):
    centre = padded[:, 1:-1, 1:-1]
    plus_z = padded[:, 2:, 1:-1]
    minus_z = padded[:, :-2, 1:-1]
    plus_y = padded[:, 1:-1, 2:]
    minus_y = padded[:, 1:-1, :-2]
    speeds = coef_pad[:3, 1:-1, 1:-1]
    laplace = plus_z + minus_z + plus_y + minus_y - 4.0 * centre
    drift = speeds[0] * (shift_cells(centre, 1) - shift_cells(centre, -1))
    drift = drift + speeds[1] * (plus_y - minus_y) + speeds[2] * (plus_z - minus_z)
    return centre + diffuse_cross * laplace - 0.5 * drift

def adjoint_explicit(padded, coef_pad):
    centre = padded[:, 1:-1, 1:-1]
    laplace = padded[:, 2:, 1:-1] + padded[:, :-2, 1:-1] + padded[:, 1:-1, 2:] + padded[:, 1:-1, :-2] - 4.0 * centre
    flux_x = coef_pad[0, 1:-1, 1:-1] * centre
    flux_y = coef_pad[1, 1:-1, :] * padded[:, 1:-1, :]
    flux_z = coef_pad[2, :, 1:-1] * padded[:, :, 1:-1]
    drift = shift_cells(flux_x, 1) - shift_cells(flux_x, -1)
    drift = drift + flux_y[:, :, 2:] - flux_y[:, :, :-2] + flux_z[:, 2:] - flux_z[:, :-2]
    return centre + diffuse_cross * laplace + 0.5 * drift

def solve_probes(work, coef_pad, matrix, padder):
    weight_src = coef_pad[3, 1:-1, 1:-1]
    weight_obs = coef_pad[4, 1:-1, 1:-1]
    source = weight_src * work
    state = apply_implicit(source, matrix)
    states = [state]
    for counter in range(1, STEPS):
        state = apply_implicit(forward_explicit(padder(state), coef_pad) + source, matrix)
        states.append(state)
    adjoint = weight_obs * states[-1]
    pulled = apply_implicit(adjoint, matrix)
    gradient = pulled
    for counter in range(STEPS - 2, -1, -1):
        adjoint = weight_obs * states[counter] + adjoint_explicit(padder(pulled), coef_pad)
        pulled = apply_implicit(adjoint, matrix)
        gradient = gradient + pulled
    return weight_src * gradient

def pad_field(field):
    return jnp.pad(field, ((0, 0), (1, 1), (1, 1), (0, 0)))

def reference(probes, velocity, prior_scale, noise_precision, source_mask, sensor_mask):
    weight_src = source_mask.astype(jnp.float32) * prior_scale
    weight_obs = sensor_mask.astype(jnp.float32) * noise_precision
    coeffs = jnp.concatenate([velocity, weight_src[None], weight_obs[None]], 0)
    coef_pad = pad_field(coeffs)
    length = probes.shape[-1]
    eye = jnp.eye(length, dtype=jnp.float32)
    banded = (1.0 + 2.0 * diffuse_along) * eye - diffuse_along * (jnp.eye(length, k=1, dtype=jnp.float32) + jnp.eye(length, k=-1, dtype=jnp.float32))
    matrix = jnp.linalg.inv(banded)
    hessian = solve_probes(probes, coef_pad, matrix, pad_field)
    count = probes.shape[0]
    cells = probes.shape[1] * probes.shape[2] * probes.shape[3]
    gram = jnp.einsum('ac,bc->ab', probes.reshape(count, -1), hessian.reshape(count, -1), precision=lax.Precision.HIGHEST) / cells
    return (hessian, gram)
```

```python
import functools

import jax
import jax.numpy as jnp
import numpy as np
from jax import lax
from jax.experimental import pallas as pl
from jax.experimental.pallas import tpu as pltpu
from jax.sharding import PartitionSpec as P

STEPS = 5
diffuse_cross = 0.15
diffuse_along = 16.0
SENDS = 2 * (STEPS - 1)
F32 = jnp.float32
BF16 = jnp.bfloat16


def matrix_parts(length):
    banded = (1.0 + 2.0 * diffuse_along) * np.eye(length) - diffuse_along * (
        np.eye(length, k=1) + np.eye(length, k=-1)
    )
    matrix = np.linalg.inv(banded)
    high = matrix.astype(BF16)
    low = (matrix - high.astype(np.float64)).astype(BF16)
    return high, low


def kernel(
    sizes,
    probes_hbm,
    vel,
    prior,
    noise,
    smask,
    omask,
    mhigh,
    mlow,
    hess_hbm,
    gram_ref,
    own,
    other,
    states,
    field,
    grad,
    half,
    wsrc,
    wobs,
    xhigh,
    xlow,
    zsend,
    zrecv,
    ysend,
    yrecv,
    gpart,
    gtile,
    grecv,
    stile,
    srecv,
    send_sem,
    recv_sem,
    load_sem,
    store_sem,
    pair_send,
    pair_recv,
    g_send,
    g_recv,
    s_send,
    s_recv,
):
    ngz, ngy, npa = sizes
    np_, nz, ny, nx = own.shape
    gz, gy, pa = lax.axis_index("gz"), lax.axis_index("gy"), lax.axis_index("pa")
    has_to = (gz < ngz - 1, gz > 0, gy < ngy - 1, gy > 0)
    has_from = (gz > 0, gz < ngz - 1, gy > 0, gy < ngy - 1)
    target = ({"gz": gz + 1}, {"gz": gz - 1}, {"gy": gy + 1}, {"gy": gy - 1})

    plane = [(dy, dp) for dy in range(ngy) for dp in range(npa) if dy or dp]

    def plane_id(dy, dp):
        return {"gy": lax.rem(gy + dy, ngy), "pa": lax.rem(pa + dp, npa)}

    def line_id(dz):
        return {"gz": lax.rem(gz + dz, ngz)}

    def load(p):
        return pltpu.make_async_copy(probes_hbm.at[p], own.at[p], load_sem.at[p])

    for p in range(np_):
        load(p).start()

    barrier = pltpu.get_barrier_semaphore()
    peers = [plane_id(dy, dp) for dy, dp in plane] + [line_id(dz) for dz in range(1, ngz)]
    for peer in peers:
        pl.semaphore_signal(barrier, inc=1, device_id=peer, device_id_type=pl.DeviceIdType.MESH)

    def prepare(z, carry):
        half[0, z] = 0.5 * vel[0, z]
        half[1, z] = 0.5 * vel[1, z]
        half[2, z] = 0.5 * vel[2, z]
        wsrc[z] = smask[z].astype(F32) * prior[z]
        wobs[z] = omask[z].astype(F32) * noise[z]
        return carry

    lax.fori_loop(0, nz, prepare, 0)

    @pl.when(jnp.logical_not(has_from[0]))
    def _():
        zrecv[:, :, 0] = jnp.zeros((2, np_, ny, nx), F32)

    @pl.when(jnp.logical_not(has_from[1]))
    def _():
        zrecv[:, :, 1] = jnp.zeros((2, np_, ny, nx), F32)

    @pl.when(jnp.logical_not(has_from[2]))
    def _():
        yrecv[:, :, 0] = jnp.zeros((2, np_, nz, nx), F32)

    @pl.when(jnp.logical_not(has_from[3]))
    def _():
        yrecv[:, :, 1] = jnp.zeros((2, np_, nz, nx), F32)

    pl.semaphore_wait(barrier, len(peers))

    def pair_copy(dp):
        return pltpu.make_async_remote_copy(
            src_ref=probes_hbm,
            dst_ref=other.at[dp - 1],
            send_sem=pair_send.at[dp - 1],
            recv_sem=pair_recv.at[dp - 1],
            device_id={"pa": lax.rem(pa + npa - dp, npa)},
            device_id_type=pl.DeviceIdType.MESH,
        )

    for dp in range(1, npa):
        pair_copy(dp).start()

    def face(d, par, p):
        send, recv = (zsend, zrecv) if d < 2 else (ysend, yrecv)
        return pltpu.make_async_remote_copy(
            src_ref=send.at[par, p, d % 2],
            dst_ref=recv.at[par, p, d % 2],
            send_sem=send_sem.at[d, par, p],
            recv_sem=recv_sem.at[d, par, p],
            device_id=target[d],
            device_id_type=pl.DeviceIdType.MESH,
        )

    def await_sent(par, p, also=None):
        for d in range(4):
            cond = has_to[d] if also is None else jnp.logical_and(has_to[d], also)

            @pl.when(cond)
            def _():
                face(d, par, p).wait_send()

    def start_faces(par, p):
        for d in range(4):

            @pl.when(has_to[d])
            def _():
                face(d, par, p).start()

    def await_faces(par, p):
        for d in range(4):

            @pl.when(has_from[d])
            def _():
                face(d, par, p).wait_recv()

    row = lax.broadcasted_iota(jnp.int32, (ny, nx), 0)
    lane = lax.broadcasted_iota(jnp.int32, (ny, nx), 1)

    def from_below_y(value, edge):
        return jnp.where(row == 0, edge, pltpu.roll(value, 1, 0))

    def from_above_y(value, edge):
        return jnp.where(row == ny - 1, edge, pltpu.roll(value, ny - 1, 0))

    def from_below_x(value):
        return jnp.where(lane == 0, 0.0, pltpu.roll(value, 1, 1))

    def from_above_x(value):
        return jnp.where(lane == nx - 1, 0.0, pltpu.roll(value, nx - 1, 1))

    def put(z, value):
        high = value.astype(BF16)
        xhigh[z * ny : (z + 1) * ny] = high
        xlow[z * ny : (z + 1) * ny] = (value - high.astype(F32)).astype(BF16)

    def implicit():
        total = jnp.dot(xhigh[...], mhigh[...], preferred_element_type=F32)
        total += jnp.dot(xlow[...], mhigh[...], preferred_element_type=F32)
        total += jnp.dot(xhigh[...], mlow[...], preferred_element_type=F32)
        return total.reshape(nz, ny, nx)

    def send_state(n, par, p):
        zsend[par, p, 0] = states[n, p, nz - 1]
        zsend[par, p, 1] = states[n, p, 0]
        for z in range(nz):
            ysend[par, p, 0, z : z + 1] = states[n, p, z, ny - 1 : ny]
            ysend[par, p, 1, z : z + 1] = states[n, p, z, 0:1]
        start_faces(par, p)

    def send_field(par, p):
        zsend[par, p, 0] = (diffuse_cross - half[2, nz - 1]) * field[p, nz - 1]
        zsend[par, p, 1] = (diffuse_cross + half[2, 0]) * field[p, 0]
        for z in range(nz):
            ysend[par, p, 0, z : z + 1] = (diffuse_cross - half[1, z, ny - 1 : ny]) * field[
                p, z, ny - 1 : ny
            ]
            ysend[par, p, 1, z : z + 1] = (diffuse_cross + half[1, z, 0:1]) * field[p, z, 0:1]
        start_faces(par, p)

    def forward(n, par, p):
        await_faces(par, p)
        for z in range(nz):
            centre = states[n, p, z]
            minus_z = states[n, p, z - 1] if z > 0 else zrecv[par, p, 0]
            plus_z = states[n, p, z + 1] if z < nz - 1 else zrecv[par, p, 1]
            minus_y = from_below_y(centre, yrecv[par, p, 0, z : z + 1])
            plus_y = from_above_y(centre, yrecv[par, p, 1, z : z + 1])
            drift = half[0, z] * (from_above_x(centre) - from_below_x(centre))
            drift += half[1, z] * (plus_y - minus_y) + half[2, z] * (plus_z - minus_z)
            cross = (plus_z + minus_z) + (plus_y + minus_y)
            moved = (1.0 - 4.0 * diffuse_cross) * centre + diffuse_cross * cross - drift
            put(z, moved + wsrc[z] * own[p, z])
        return implicit()

    def adjoint(n, par, p):
        await_faces(par, p)

        def split_z(z):
            value = field[p, z]
            flux = half[2, z] * value
            value = diffuse_cross * value
            return value + flux, value - flux

        below = zrecv[par, p, 0]
        here = split_z(0)
        for z in range(nz):
            above = split_z(z + 1) if z < nz - 1 else (zrecv[par, p, 1], None)
            centre = field[p, z]
            scaled = diffuse_cross * centre
            flux_y = half[1, z] * centre
            flux_x = half[0, z] * centre
            total = (1.0 - 4.0 * diffuse_cross) * centre + wobs[z] * states[n, p, z]
            total += above[0] + below
            total += from_above_y(scaled + flux_y, yrecv[par, p, 1, z : z + 1])
            total += from_below_y(scaled - flux_y, yrecv[par, p, 0, z : z + 1])
            total += from_above_x(flux_x) - from_below_x(flux_x)
            put(z, total)
            below = here[1]
            here = above
        return implicit()

    def first(p, carry):
        load(p).wait()
        for z in range(nz):
            put(z, wsrc[z] * own[p, z])
        states[0, p] = implicit()
        send_state(0, 0, p)
        return carry

    lax.fori_loop(0, np_, first, 0)

    def forward_step(index, carry):
        n, p = index // np_, lax.rem(index, np_)
        par = lax.rem(n, 2)
        states[n + 1, p] = forward(n, par, p)
        await_sent(1 - par, p, n >= 1)
        send_state(n + 1, 1 - par, p)
        return carry

    lax.fori_loop(0, (STEPS - 2) * np_, forward_step, 0)

    def turn(p, carry):
        par = (STEPS - 2) % 2
        last = forward(STEPS - 2, par, p)
        for z in range(nz):
            put(z, wobs[z] * last[z])
        pulled = implicit()
        field[p] = pulled
        grad[p] = pulled
        await_sent(1 - par, p)
        send_field(1 - par, p)
        return carry

    lax.fori_loop(0, np_, turn, 0)

    def adjoint_step(index, carry):
        step, p = index // np_, lax.rem(index, np_)
        par = lax.rem(step + STEPS - 1, 2)
        pulled = adjoint(STEPS - 2 - step, par, p)
        field[p] = pulled
        grad[p] = grad[p] + pulled
        await_sent(1 - par, p)
        send_field(1 - par, p)
        return carry

    lax.fori_loop(0, (STEPS - 2) * np_, adjoint_step, 0)

    for dp in range(1, npa):
        pair_copy(dp).wait()

    def store(p):
        return pltpu.make_async_copy(grad.at[p], hess_hbm.at[p], store_sem.at[p])

    def fold(value):
        return functools.reduce(jnp.add, [value[y : y + 8] for y in range(0, ny, 8)])

    def finish(p, carry):
        pulled = adjoint(0, (SENDS - 1) % 2, p)
        grad[p] = wsrc[...] * (grad[p] + pulled)
        store(p).start()
        for dp in range(npa):
            sums = [None] * np_
            for z in range(nz):
                action = grad[p, z]
                for i in range(np_):
                    probe = own[i, z] if dp == 0 else other[dp - 1, i, z]
                    term = fold(probe * action)
                    sums[i] = term if sums[i] is None else sums[i] + term
            for i in range(np_):
                part = functools.reduce(
                    jnp.add, [sums[i][:, x : x + 128] for x in range(0, nx, 128)]
                )
                gpart[dp, p, i : i + 1] = jnp.sum(part, axis=0, keepdims=True)
        return carry

    lax.fori_loop(0, np_, finish, 0)

    column = lax.broadcasted_iota(jnp.int32, (np_, 128), 1)
    for dp in range(npa):
        tile = jnp.zeros((np_, 128), F32)
        for j in range(np_):
            sums = jnp.sum(gpart[dp, j], axis=1, keepdims=True)
            tile = jnp.where(column == pa * np_ + j, sums, tile)
        gtile[dp] = tile

    def plane_copy(k):
        dy, dp = plane[k]
        return pltpu.make_async_remote_copy(
            src_ref=gtile.at[dp],
            dst_ref=grecv.at[k],
            send_sem=g_send.at[k],
            recv_sem=g_recv.at[k],
            device_id=plane_id(dy, dp),
            device_id_type=pl.DeviceIdType.MESH,
        )

    def line_copy(dz):
        return pltpu.make_async_remote_copy(
            src_ref=stile,
            dst_ref=srecv.at[dz - 1],
            send_sem=s_send.at[dz - 1],
            recv_sem=s_recv.at[dz - 1],
            device_id=line_id(dz),
            device_id_type=pl.DeviceIdType.MESH,
        )

    for k in range(len(plane)):
        plane_copy(k).start()
    total = gtile[0]
    for k in range(len(plane)):
        plane_copy(k).wait_recv()
        total += grecv[k]
    stile[...] = total
    for dz in range(1, ngz):
        line_copy(dz).start()
    for k in range(len(plane)):
        plane_copy(k).wait_send()

    def drain(p, carry):
        store(p).wait()
        await_sent(0, p)
        await_sent(1, p)
        return carry

    lax.fori_loop(0, np_, drain, 0)

    for dz in range(1, ngz):
        line_copy(dz).wait_recv()
        total += srecv[dz - 1]
    for dz in range(1, ngz):
        line_copy(dz).wait_send()
    cells = nz * ny * nx * ngz * ngy
    gram_ref[...] = total[:, : npa * np_] / cells


def shards(probes, velocity, prior_scale, noise_precision, source_mask, sensor_mask):
    np_, nz, ny, nx = probes.shape
    ngz, ngy, npa = lax.axis_size("gz"), lax.axis_size("gy"), lax.axis_size("pa")
    high, low = matrix_parts(nx)
    plane = ngy * npa - 1
    vmem = pl.BlockSpec(memory_space=pltpu.VMEM)
    hbm = pl.BlockSpec(memory_space=pl.ANY)
    dma = pltpu.SemaphoreType.DMA
    return pl.pallas_call(
        functools.partial(kernel, (ngz, ngy, npa)),
        out_shape=(
            jax.ShapeDtypeStruct(probes.shape, F32),
            jax.ShapeDtypeStruct((np_, npa * np_), F32),
        ),
        in_specs=[hbm] + [vmem] * 7,
        out_specs=(hbm, vmem),
        scratch_shapes=[
            pltpu.VMEM((np_, nz, ny, nx), F32),
            pltpu.VMEM((npa - 1, np_, nz, ny, nx), F32),
            pltpu.VMEM((STEPS - 1, np_, nz, ny, nx), F32),
            pltpu.VMEM((np_, nz, ny, nx), F32),
            pltpu.VMEM((np_, nz, ny, nx), F32),
            pltpu.VMEM((3, nz, ny, nx), F32),
            pltpu.VMEM((nz, ny, nx), F32),
            pltpu.VMEM((nz, ny, nx), F32),
            pltpu.VMEM((nz * ny, nx), BF16),
            pltpu.VMEM((nz * ny, nx), BF16),
            pltpu.VMEM((2, np_, 2, ny, nx), F32),
            pltpu.VMEM((2, np_, 2, ny, nx), F32),
            pltpu.VMEM((2, np_, 2, nz, nx), F32),
            pltpu.VMEM((2, np_, 2, nz, nx), F32),
            pltpu.VMEM((npa, np_, np_, 128), F32),
            pltpu.VMEM((npa, np_, 128), F32),
            pltpu.VMEM((plane, np_, 128), F32),
            pltpu.VMEM((np_, 128), F32),
            pltpu.VMEM((ngz - 1, np_, 128), F32),
            dma((4, 2, np_)),
            dma((4, 2, np_)),
            dma((np_,)),
            dma((np_,)),
            dma((npa - 1,)),
            dma((npa - 1,)),
            dma((plane,)),
            dma((plane,)),
            dma((ngz - 1,)),
            dma((ngz - 1,)),
        ],
        compiler_params=pltpu.CompilerParams(
            collective_id=0, has_side_effects=True, vmem_limit_bytes=48 * 1024 * 1024
        ),
    )(
        probes,
        velocity,
        prior_scale,
        noise_precision,
        source_mask,
        sensor_mask,
        jnp.asarray(high),
        jnp.asarray(low),
    )


def solution(mesh):
    in_specs = (
        P(("chain", "pa"), "gz", "gy", None),
        P(None, ("chain", "gz"), "gy", None),
        P(("chain", "gz"), "gy", None),
        P(("chain", "gz"), "gy", None),
        P(("chain", "gz"), "gy", None),
        P(("chain", "gz"), "gy", None),
    )
    out_specs = (P(("chain", "pa"), "gz", "gy", None), P(("chain", "pa"), None))
    return jax.shard_map(shards, mesh=mesh, in_specs=in_specs, out_specs=out_specs, check_vma=False)
```

```python
import functools

import jax
import jax.numpy as jnp
import numpy as np
from jax import lax
from jax.experimental import pallas as pl
from jax.experimental.pallas import tpu as pltpu
from jax.sharding import PartitionSpec as P

STEPS = 5
diffuse_cross = 0.15
diffuse_along = 16.0
SENDS = 2 * (STEPS - 1)
F32 = jnp.float32
BF16 = jnp.bfloat16


def matrix_parts(length):
    banded = (1.0 + 2.0 * diffuse_along) * np.eye(length) - diffuse_along * (
        np.eye(length, k=1) + np.eye(length, k=-1)
    )
    matrix = np.linalg.inv(banded)
    high = matrix.astype(BF16)
    low = (matrix - high.astype(np.float64)).astype(BF16)
    return high, low


def kernel(
    sizes,
    probes_hbm,
    vel_hbm,
    prior_hbm,
    noise_hbm,
    smask_hbm,
    omask_hbm,
    mhigh_hbm,
    mlow_hbm,
    hess_hbm,
    gram_ref,
    own,
    other,
    states,
    field,
    grad,
    moved2,
    half,
    wsrc,
    wobs,
    smask,
    omask,
    mhigh,
    mlow,
    xhigh,
    xlow,
    zsend,
    zrecv,
    ysend,
    yrecv,
    gpart,
    gtile,
    grecv,
    stile,
    srecv,
    send_sem,
    recv_sem,
    load_sem,
    coef_sem,
    store_sem,
    pair_send,
    pair_recv,
    g_send,
    g_recv,
    s_send,
    s_recv,
):
    ngz, ngy, npa = sizes
    np_, nz, ny, nx = own.shape
    gz, gy, pa = lax.axis_index("gz"), lax.axis_index("gy"), lax.axis_index("pa")
    has_to = (gz < ngz - 1, gz > 0, gy < ngy - 1, gy > 0)
    has_from = (gz > 0, gz < ngz - 1, gy > 0, gy < ngy - 1)
    target = ({"gz": gz + 1}, {"gz": gz - 1}, {"gy": gy + 1}, {"gy": gy - 1})

    plane = [(dy, dp) for dy in range(ngy) for dp in range(npa) if dy or dp]

    def plane_id(dy, dp):
        return {"gy": lax.rem(gy + dy, ngy), "pa": lax.rem(pa + dp, npa)}

    def line_id(dz):
        return {"gz": lax.rem(gz + dz, ngz)}

    def load(p):
        return pltpu.make_async_copy(probes_hbm.at[p], own.at[p], load_sem.at[p])

    coefs = [
        (smask_hbm, smask),
        (prior_hbm, wsrc),
        (mhigh_hbm, mhigh),
        (mlow_hbm, mlow),
        (vel_hbm, half),
        (omask_hbm, omask),
        (noise_hbm, wobs),
    ]

    def coef(k):
        return pltpu.make_async_copy(coefs[k][0], coefs[k][1], coef_sem.at[k])

    for k in range(4):
        coef(k).start()
    load(0).start()
    load(1).start()
    for k in range(4, len(coefs)):
        coef(k).start()
    for p in range(2, np_):
        load(p).start()

    barrier = pltpu.get_barrier_semaphore()
    peers = [plane_id(dy, dp) for dy, dp in plane] + [line_id(dz) for dz in range(1, ngz)]
    for peer in peers:
        pl.semaphore_signal(barrier, inc=1, device_id=peer, device_id_type=pl.DeviceIdType.MESH)

    @pl.when(jnp.logical_not(has_from[0]))
    def _():
        zrecv[:, :, 0] = jnp.zeros((2, np_, ny, nx), F32)

    @pl.when(jnp.logical_not(has_from[1]))
    def _():
        zrecv[:, :, 1] = jnp.zeros((2, np_, ny, nx), F32)

    @pl.when(jnp.logical_not(has_from[2]))
    def _():
        yrecv[:, :, 0] = jnp.zeros((2, np_, nz, nx), F32)

    @pl.when(jnp.logical_not(has_from[3]))
    def _():
        yrecv[:, :, 1] = jnp.zeros((2, np_, nz, nx), F32)

    for k in range(4):
        coef(k).wait()

    def prepare_source(z, carry):
        wsrc[z] = smask[z].astype(F32) * wsrc[z]
        return carry

    lax.fori_loop(0, nz, prepare_source, 0)

    pl.semaphore_wait(barrier, len(peers))

    pair_sources = (probes_hbm, states.at[0], moved2)

    def pair_copy(dp, k):
        return pltpu.make_async_remote_copy(
            src_ref=pair_sources[k],
            dst_ref=other.at[dp - 1, k],
            send_sem=pair_send.at[dp - 1, k],
            recv_sem=pair_recv.at[dp - 1, k],
            device_id={"pa": lax.rem(pa + npa - dp, npa)},
            device_id_type=pl.DeviceIdType.MESH,
        )

    def start_pairs(k):
        for dp in range(1, npa):
            pair_copy(dp, k).start()

    def await_pairs(k):
        for dp in range(1, npa):
            pair_copy(dp, k).wait()

    def face(d, par, p):
        send, recv = (zsend, zrecv) if d < 2 else (ysend, yrecv)
        return pltpu.make_async_remote_copy(
            src_ref=send.at[par, p, d % 2],
            dst_ref=recv.at[par, p, d % 2],
            send_sem=send_sem.at[d, par, p],
            recv_sem=recv_sem.at[d, par, p],
            device_id=target[d],
            device_id_type=pl.DeviceIdType.MESH,
        )

    def await_sent(par, p, also=None):
        for d in range(4):
            cond = has_to[d] if also is None else jnp.logical_and(has_to[d], also)

            @pl.when(cond)
            def _():
                face(d, par, p).wait_send()

    def start_faces(par, p):
        for d in range(4):

            @pl.when(has_to[d])
            def _():
                face(d, par, p).start()

    def await_faces(par, p):
        for d in range(4):

            @pl.when(has_from[d])
            def _():
                face(d, par, p).wait_recv()

    row = lax.broadcasted_iota(jnp.int32, (ny, nx), 0)
    lane = lax.broadcasted_iota(jnp.int32, (ny, nx), 1)

    def from_below_y(value, edge):
        return jnp.where(row == 0, edge, pltpu.roll(value, 1, 0))

    def from_above_y(value, edge):
        return jnp.where(row == ny - 1, edge, pltpu.roll(value, ny - 1, 0))

    def from_below_x(value):
        return jnp.where(lane == 0, 0.0, pltpu.roll(value, 1, 1))

    def from_above_x(value):
        return jnp.where(lane == nx - 1, 0.0, pltpu.roll(value, nx - 1, 1))

    def put(z, value):
        high = value.astype(BF16)
        xhigh[z * ny : (z + 1) * ny] = high
        xlow[z * ny : (z + 1) * ny] = (value - high.astype(F32)).astype(BF16)

    def implicit():
        total = jnp.dot(xhigh[...], mhigh[...], preferred_element_type=F32)
        total += jnp.dot(xlow[...], mhigh[...], preferred_element_type=F32)
        total += jnp.dot(xhigh[...], mlow[...], preferred_element_type=F32)
        return total.reshape(nz, ny, nx)

    def send_state(n, par, p):
        zsend[par, p, 0] = states[n, p, nz - 1]
        zsend[par, p, 1] = states[n, p, 0]
        for z in range(nz):
            ysend[par, p, 0, z : z + 1] = states[n, p, z, ny - 1 : ny]
            ysend[par, p, 1, z : z + 1] = states[n, p, z, 0:1]
        start_faces(par, p)

    def send_field(par, p):
        zsend[par, p, 0] = (diffuse_cross - half[2, nz - 1]) * field[p, nz - 1]
        zsend[par, p, 1] = (diffuse_cross + half[2, 0]) * field[p, 0]
        for z in range(nz):
            ysend[par, p, 0, z : z + 1] = (diffuse_cross - half[1, z, ny - 1 : ny]) * field[
                p, z, ny - 1 : ny
            ]
            ysend[par, p, 1, z : z + 1] = (diffuse_cross + half[1, z, 0:1]) * field[p, z, 0:1]
        start_faces(par, p)

    def forward(n, par, p, keep=False):
        await_faces(par, p)
        for z in range(nz):
            centre = states[n, p, z]
            minus_z = states[n, p, z - 1] if z > 0 else zrecv[par, p, 0]
            plus_z = states[n, p, z + 1] if z < nz - 1 else zrecv[par, p, 1]
            minus_y = from_below_y(centre, yrecv[par, p, 0, z : z + 1])
            plus_y = from_above_y(centre, yrecv[par, p, 1, z : z + 1])
            drift = half[0, z] * (from_above_x(centre) - from_below_x(centre))
            drift += half[1, z] * (plus_y - minus_y) + half[2, z] * (plus_z - minus_z)
            cross = (plus_z + minus_z) + (plus_y + minus_y)
            moved = (1.0 - 4.0 * diffuse_cross) * centre + diffuse_cross * cross - drift
            moved += wsrc[z] * own[p, z]
            if keep:
                moved2[p, z] = moved
            put(z, moved)
        return implicit()

    def adjoint(n, par, p):
        await_faces(par, p)

        def split_z(z):
            value = field[p, z]
            flux = half[2, z] * value
            value = diffuse_cross * value
            return value + flux, value - flux

        below = zrecv[par, p, 0]
        here = split_z(0)
        for z in range(nz):
            above = split_z(z + 1) if z < nz - 1 else (zrecv[par, p, 1], None)
            centre = field[p, z]
            scaled = diffuse_cross * centre
            flux_y = half[1, z] * centre
            flux_x = half[0, z] * centre
            total = (1.0 - 4.0 * diffuse_cross) * centre + wobs[z] * states[n, p, z]
            total += above[0] + below
            total += from_above_y(scaled + flux_y, yrecv[par, p, 1, z : z + 1])
            total += from_below_y(scaled - flux_y, yrecv[par, p, 0, z : z + 1])
            total += from_above_x(flux_x) - from_below_x(flux_x)
            put(z, total)
            below = here[1]
            here = above
        return implicit()

    def first(p, carry):
        load(p).wait()
        for z in range(nz):
            put(z, wsrc[z] * own[p, z])
        states[0, p] = implicit()
        send_state(0, 0, p)
        return carry

    lax.fori_loop(0, np_, first, 0)
    start_pairs(0)

    for k in range(4, len(coefs)):
        coef(k).wait()

    def prepare(z, carry):
        for k in range(3):
            half[k, z] = 0.5 * half[k, z]
        wobs[z] = omask[z].astype(F32) * wobs[z]
        return carry

    lax.fori_loop(0, nz, prepare, 0)

    def second(p, carry):
        states[1, p] = forward(0, 0, p, True)
        send_state(1, 1, p)
        return carry

    lax.fori_loop(0, np_, second, 0)
    start_pairs(1)
    start_pairs(2)

    def forward_step(index, carry):
        n, p = index // np_ + 1, lax.rem(index, np_)
        par = lax.rem(n, 2)
        states[n + 1, p] = forward(n, par, p)
        await_sent(1 - par, p)
        send_state(n + 1, 1 - par, p)
        return carry

    lax.fori_loop(0, (STEPS - 3) * np_, forward_step, 0)

    def turn(p, carry):
        par = (STEPS - 2) % 2
        last = forward(STEPS - 2, par, p)
        for z in range(nz):
            put(z, wobs[z] * last[z])
        pulled = implicit()
        field[p] = pulled
        grad[p] = pulled
        await_sent(1 - par, p)
        send_field(1 - par, p)
        return carry

    lax.fori_loop(0, np_, turn, 0)

    def fold(value):
        return functools.reduce(jnp.add, [value[y : y + 8] for y in range(0, ny, 8)])

    def gram_term(k, p, begin):
        for dp in range(npa):
            sums = [None] * np_
            for z in range(nz):
                if k == 0:
                    right = wsrc[z] * grad[p, z]
                elif k == 1:
                    right = wobs[z] * states[0, p, z]
                else:
                    right = field[p, z]
                for i in range(np_):
                    if dp > 0:
                        left = other[dp - 1, k, i, z]
                    elif k == 0:
                        left = own[i, z]
                    elif k == 1:
                        left = states[0, i, z]
                    else:
                        left = moved2[i, z]
                    term = fold(left * right)
                    sums[i] = term if sums[i] is None else sums[i] + term
            for i in range(np_):
                part = functools.reduce(
                    jnp.add, [sums[i][:, x : x + 128] for x in range(0, nx, 128)]
                )
                part = jnp.sum(part, axis=0, keepdims=True)
                if not begin:
                    part += gpart[dp, p, i : i + 1]
                gpart[dp, p, i : i + 1] = part

    for step in range(STEPS - 2):
        par = (step + STEPS - 1) % 2
        last = step == STEPS - 3
        term = 2 if last else 0 if step == STEPS - 4 else 1 if step == 0 else None
        if term is not None:
            await_pairs(term)

        def adjoint_step(p, carry):
            pulled = adjoint(STEPS - 2 - step, par, p)
            field[p] = pulled
            grad[p] = grad[p] + pulled
            await_sent(1 - par, p)
            send_field(1 - par, p)
            if term is not None:
                gram_term(term, p, term == 1)
            return carry

        lax.fori_loop(0, np_, adjoint_step, 0)

    def store(p):
        return pltpu.make_async_copy(grad.at[p], hess_hbm.at[p], store_sem.at[p])

    def finish(p, carry):
        pulled = adjoint(0, (SENDS - 1) % 2, p)
        grad[p] = wsrc[...] * (grad[p] + pulled)
        store(p).start()
        return carry

    column = lax.broadcasted_iota(jnp.int32, (np_, 128), 1)
    for dp in range(npa):
        tile = jnp.zeros((np_, 128), F32)
        for j in range(np_):
            sums = jnp.sum(gpart[dp, j], axis=1, keepdims=True)
            tile = jnp.where(column == pa * np_ + j, sums, tile)
        gtile[dp] = tile

    def plane_copy(k):
        dy, dp = plane[k]
        return pltpu.make_async_remote_copy(
            src_ref=gtile.at[dp],
            dst_ref=grecv.at[k],
            send_sem=g_send.at[k],
            recv_sem=g_recv.at[k],
            device_id=plane_id(dy, dp),
            device_id_type=pl.DeviceIdType.MESH,
        )

    def line_copy(dz):
        return pltpu.make_async_remote_copy(
            src_ref=stile,
            dst_ref=srecv.at[dz - 1],
            send_sem=s_send.at[dz - 1],
            recv_sem=s_recv.at[dz - 1],
            device_id=line_id(dz),
            device_id_type=pl.DeviceIdType.MESH,
        )

    for k in range(len(plane)):
        plane_copy(k).start()
    lax.fori_loop(0, np_ // 4, finish, 0)
    total = gtile[0]
    for k in range(len(plane)):
        plane_copy(k).wait_recv()
        total += grecv[k]
    stile[...] = total
    for dz in range(1, ngz):
        line_copy(dz).start()
    for k in range(len(plane)):
        plane_copy(k).wait_send()
    lax.fori_loop(np_ // 4, np_, finish, 0)

    def drain(p, carry):
        store(p).wait()
        await_sent(0, p)
        await_sent(1, p)
        return carry

    lax.fori_loop(0, np_, drain, 0)

    total = stile[...]
    for dz in range(1, ngz):
        line_copy(dz).wait_recv()
        total += srecv[dz - 1]
    for dz in range(1, ngz):
        line_copy(dz).wait_send()
    cells = nz * ny * nx * ngz * ngy
    gram_ref[...] = total[:, : npa * np_] / cells


def shards(probes, velocity, prior_scale, noise_precision, source_mask, sensor_mask):
    np_, nz, ny, nx = probes.shape
    ngz, ngy, npa = lax.axis_size("gz"), lax.axis_size("gy"), lax.axis_size("pa")
    high, low = matrix_parts(nx)
    plane = ngy * npa - 1
    vmem = pl.BlockSpec(memory_space=pltpu.VMEM)
    hbm = pl.BlockSpec(memory_space=pl.ANY)
    dma = pltpu.SemaphoreType.DMA
    return pl.pallas_call(
        functools.partial(kernel, (ngz, ngy, npa)),
        out_shape=(
            jax.ShapeDtypeStruct(probes.shape, F32),
            jax.ShapeDtypeStruct((np_, npa * np_), F32),
        ),
        in_specs=[hbm] * 8,
        out_specs=(hbm, vmem),
        scratch_shapes=[
            pltpu.VMEM((np_, nz, ny, nx), F32),
            pltpu.VMEM((npa - 1, 3, np_, nz, ny, nx), F32),
            pltpu.VMEM((STEPS - 1, np_, nz, ny, nx), F32),
            pltpu.VMEM((np_, nz, ny, nx), F32),
            pltpu.VMEM((np_, nz, ny, nx), F32),
            pltpu.VMEM((np_, nz, ny, nx), F32),
            pltpu.VMEM((3, nz, ny, nx), F32),
            pltpu.VMEM((nz, ny, nx), F32),
            pltpu.VMEM((nz, ny, nx), F32),
            pltpu.VMEM((nz, ny, nx), jnp.int32),
            pltpu.VMEM((nz, ny, nx), jnp.int32),
            pltpu.VMEM((nx, nx), BF16),
            pltpu.VMEM((nx, nx), BF16),
            pltpu.VMEM((nz * ny, nx), BF16),
            pltpu.VMEM((nz * ny, nx), BF16),
            pltpu.VMEM((2, np_, 2, ny, nx), F32),
            pltpu.VMEM((2, np_, 2, ny, nx), F32),
            pltpu.VMEM((2, np_, 2, nz, nx), F32),
            pltpu.VMEM((2, np_, 2, nz, nx), F32),
            pltpu.VMEM((npa, np_, np_, 128), F32),
            pltpu.VMEM((npa, np_, 128), F32),
            pltpu.VMEM((plane, np_, 128), F32),
            pltpu.VMEM((np_, 128), F32),
            pltpu.VMEM((ngz - 1, np_, 128), F32),
            dma((4, 2, np_)),
            dma((4, 2, np_)),
            dma((np_,)),
            dma((7,)),
            dma((np_,)),
            dma((npa - 1, 3)),
            dma((npa - 1, 3)),
            dma((plane,)),
            dma((plane,)),
            dma((ngz - 1,)),
            dma((ngz - 1,)),
        ],
        compiler_params=pltpu.CompilerParams(
            collective_id=0, has_side_effects=True, vmem_limit_bytes=62 * 1024 * 1024
        ),
    )(
        probes,
        velocity,
        prior_scale,
        noise_precision,
        source_mask,
        sensor_mask,
        jnp.asarray(high),
        jnp.asarray(low),
    )


def solution(mesh):
    in_specs = (
        P(("chain", "pa"), "gz", "gy", None),
        P(None, ("chain", "gz"), "gy", None),
        P(("chain", "gz"), "gy", None),
        P(("chain", "gz"), "gy", None),
        P(("chain", "gz"), "gy", None),
        P(("chain", "gz"), "gy", None),
    )
    out_specs = (P(("chain", "pa"), "gz", "gy", None), P(("chain", "pa"), None))
    return jax.shard_map(shards, mesh=mesh, in_specs=in_specs, out_specs=out_specs, check_vma=False)
```
